32 devices in a mesh: cells: 16 (over z, x, core), ens: 2 (over y).
Axes of the slice: x: 2, y: 2, z: 4, core: 2. Of those that a mesh axis runs over, the one named last changes fastest.
Arguments:
- later_adjoint: float32 [4, 4, 32, 8, 128], P('ens', None, 'cells'), may hold values from -6 to 6
- coupling: bfloat16 [4, 6, 4, 4, 32, 8, 128], P('ens', None, None, None, 'cells'), may hold values from -0.59765625 to 0.59765625
- diag_inverse: bfloat16 [4, 4, 4, 32, 8, 128], P('ens', None, None, 'cells'), may hold values from -0.7 to 1.6, as said below
- sensitivity: bfloat16 [4, 4, 32, 8, 128, 128], P('ens', None, 'cells'), may hold values from -0.0625 to 0.0625
- well_cells: int32 [256], replicated, may hold values from 0 to 32767
- well_misfit: float32 [4, 4, 256], P('ens'), may hold values from -6 to 6
- block_map: int32 [32, 8, 128], P('cells'), may hold values from 0 to 63, as said below
Outputs:
- adjoint: float32 [4, 4, 32, 8, 128], P('ens', None, 'cells')
- gradient: float32 [64, 128], P('cells')
The draws below stay inside these ranges and needn't reach their ends.
Inputs may be any that keep to these rules, and one draw needn't show every extreme that they name: `block_map`: of the cells of each slab of 2 planes along the first dimension (x from i * 2 to i * 2 + 1), exactly 128 map to blocks whose number divided by 4 (rounded down) equals any given j. `diag_inverse`: each block is the inverse of a diagonal block; its diagonal entries lie in 0.4 to 1.6. `well_cells`: wells may share a cell.
All inputs are finite; a program needn't handle non-finite values.
Results may differ from the reference program's by a relative error of at most 0.0003.
Values sent between devices are 32-bit elements; how exact they have to be, the bound alone decides.
A program may use at most 64 MiB of HBM per device.

```python
import jax
import jax.numpy as jnp
from jax import lax

UNK = 4
PBLK = 128
CX = 2
NY = 8
NZ = 128
ITERS = 4
WELLS = 256
BLK_DEV = 4
MEMBERS = 4
NX = 32
NBLK = 64
N_CELLS = 16


def draw_diag_inverse(key, part):
    shape = (MEMBERS, UNK, UNK, NX, NY, NZ)
    identity = jnp.eye(UNK, dtype=jnp.float32)[None, :, :, None, None, None]
    key_diag = jax.random.fold_in(key, 21)
    key_off = jax.random.fold_in(key, 22)
    diagonal = jax.random.uniform(key_diag, shape, jnp.float32, 0.6, 1.4)
    offdiag = jnp.clip(0.2 * jax.random.normal(key_off, shape, jnp.float32), -0.7, 0.7)
    return (identity * diagonal + (1.0 - identity) * offdiag).astype(jnp.bfloat16)


def draw_block_map(key, part):
    slab_cells = CX * NY * NZ
    per_owner = slab_cells // N_CELLS
    owners = jnp.repeat(jnp.arange(N_CELLS, dtype=jnp.int32), per_owner)
    keys = jax.random.split(jax.random.fold_in(key, 31), N_CELLS)
    shuffled = jax.vmap(lambda single: jax.random.permutation(single, owners))(keys)
    within = jax.random.randint(jax.random.fold_in(key, 32), (N_CELLS, slab_cells), 0, BLK_DEV, dtype=jnp.int32)
    return (shuffled * BLK_DEV + within).reshape(NX, NY, NZ)


def plant(entries, stream_key, low, high):
    longest = entries.shape.index(max(entries.shape))
    spots = []
    for shift in (0, 1):
        where = [jax.random.randint(jax.random.fold_in(stream_key, axis), (), 0, length) for axis, length in enumerate(entries.shape)]
        where[longest] = (where[longest] + shift) % entries.shape[longest]
        spots.append(tuple(where))
    return entries.at[spots[0]].set(low).at[spots[1]].set(high)


def level_of(rng, shape, cuts, smallest, largest):
    def one(position, blocks):
        heights = jax.random.uniform(jax.random.fold_in(jax.random.fold_in(rng, 6), position), (blocks,), jnp.float32, smallest / len(cuts), largest / len(cuts))
        return jnp.repeat(jnp.exp(heights), shape[position] // blocks).reshape((-1,) + (1,) * (len(shape) - position - 1))

    loudness = one(*cuts[0])
    for cut in cuts[1:]:
        loudness = loudness * one(*cut)
    return loudness


def scatter_about(own_key, shape, width, most, cuts=(), kind=jnp.bfloat16):
    factor_of = level_of(own_key, shape, cuts, -0.22, 0.18) if cuts else 1.0
    result = jax.random.normal(own_key, shape, jnp.float32) * width * factor_of
    return jnp.minimum(jnp.maximum(result, -most), most).astype(kind)


def setup_inputs(seed: int = 0) -> dict:
    splits = jax.random.split(jax.random.key(seed), 8)
    later_adjoint = scatter_about(splits[0], (MEMBERS, UNK, NX, NY, NZ), 1.0, 6.0, ((0, 2), (2, 16)), jnp.float32)
    coupling = scatter_about(splits[1], (MEMBERS, 6, UNK, UNK, NX, NY, NZ), 0.1, 0.59765625, ((0, 2), (4, 16)))
    diag_inverse = draw_diag_inverse(jax.random.fold_in(splits[7], 71), 0)
    sensitivity = scatter_about(splits[3], (MEMBERS, UNK, NX, NY, NZ, PBLK), (UNK * MEMBERS * CX * NY * NZ // BLK_DEV) ** -0.5, 0.0625, ((0, 2), (2, 16)))
    well_cells = plant(jax.random.randint(splits[4], (WELLS,), 0, NX * NY * NZ), jax.random.fold_in(splits[4], 1), 0, (NX * NY * NZ) - 1).astype(jnp.int32)
    well_misfit = scatter_about(splits[5], (MEMBERS, UNK, WELLS), 1.0, 6.0, ((0, 2),), jnp.float32)
    block_map = draw_block_map(jax.random.fold_in(splits[7], 71), 0)
    return {"later_adjoint": later_adjoint, "coupling": coupling, "diag_inverse": diag_inverse, "sensitivity": sensitivity, "well_cells": well_cells, "well_misfit": well_misfit, "block_map": block_map}


def move_along(field, axis, forward):
    length = field.shape[axis]
    shape = list(field.shape)
    shape[axis] = 1
    zeros = jnp.zeros(shape, jnp.float32)
    if forward:
        return jnp.concatenate([zeros, lax.slice_in_dim(field, 0, length - 1, axis=axis)], axis=axis)
    return jnp.concatenate([lax.slice_in_dim(field, 1, length, axis=axis), zeros], axis=axis)


def coupling_sum(adjoint, coupling):
    terms = jnp.sum(coupling.astype(jnp.float32) * adjoint[:, None, :, None], axis=2)
    total = jnp.zeros(adjoint.shape, jnp.float32)
    directions = [(2, True), (2, False), (3, True), (3, False), (4, True), (4, False)]
    for number, (axis, forward) in enumerate(directions):
        total = total + move_along(terms[:, number], axis, forward)
    return total


def apply_inverse(diag_inverse, source):
    return jnp.sum(diag_inverse.astype(jnp.float32) * source[:, :, None], axis=1)


def reference(later_adjoint, coupling, diag_inverse, sensitivity, well_cells, well_misfit, block_map):
    members = later_adjoint.shape[0]
    count = NX * NY * NZ
    flat = later_adjoint.reshape(members, UNK, count)
    flat = flat.at[:, :, well_cells].add(well_misfit)
    source = flat.reshape(later_adjoint.shape)
    adjoint = apply_inverse(diag_inverse, source)
    for sweep in range(ITERS):
        adjoint = apply_inverse(diag_inverse, source - coupling_sum(adjoint, coupling))
    adjoint_flat = adjoint.reshape(members, UNK, count)
    sens_flat = sensitivity.reshape(members, UNK, count, PBLK)
    cell_grad = jnp.zeros((count, PBLK), jnp.float32)
    for member in range(members):
        for unknown in range(UNK):
            cell_grad = cell_grad + adjoint_flat[member, unknown][:, None] * sens_flat[member, unknown].astype(jnp.float32)
    gradient = jax.ops.segment_sum(cell_grad, block_map.reshape(-1), num_segments=NBLK)
    return adjoint, gradient
```

```python
import functools

import jax
import jax.numpy as jnp
from jax import lax
from jax.experimental import pallas as pl
from jax.experimental.pallas import tpu as pltpu
from jax.sharding import PartitionSpec as P

ITERS = 4
MESH = pl.DeviceIdType.MESH
F32 = jnp.float32
BF16 = jnp.bfloat16


def for_each(count, step):
    if count <= 64:
        for i in range(count):
            step(i)
    else:
        def body(i, carry):
            step(i)
            return carry

        lax.fori_loop(0, count, body, 0)


def split(value):
    high = value.astype(BF16).astype(F32)
    return high, value - high


def kernel(
    ranks, groups, blocks,
    later_hbm, coup_hbm, diag_hbm, sens_hbm, wells_hbm, misfit_hbm, map_hbm,
    adj_hbm, grad_ref,
    later, coup, diag, sens, wells, misfit, bmap, adj, source,
    up_send, down_send, below, above, mask, lhs, part, got,
    load_sem, sens_sem, adj_sem, up_ssem, up_rsem, down_ssem, down_rsem, part_ssem, part_rsem,
):
    members, unknowns, planes, columns, layers = later.shape
    rows = planes * columns
    count = rows * layers
    devices = ranks * groups
    blk_dev = blocks // ranks
    me_c = lax.axis_index("cells")
    me_e = lax.axis_index("ens")
    me = me_c * groups + me_e

    def other(step):
        at = me + step + 1
        at = jnp.where(at >= devices, at - devices, at)
        return at // groups, at % groups

    barrier = pltpu.get_barrier_semaphore()

    def greet(step):
        c, e = other(step)
        pl.semaphore_signal(barrier, inc=1, device_id=(c, e), device_id_type=MESH)

    loads = [
        pltpu.make_async_copy(src, dst, load_sem.at[i])
        for i, (src, dst) in enumerate(
            [
                (wells_hbm, wells), (misfit_hbm, misfit), (later_hbm, later), (diag_hbm, diag),
                (coup_hbm, coup), (map_hbm, bmap),
            ]
        )
    ]
    for load in loads:
        load.start()
    fields = members * unknowns
    sens_loads = [
        pltpu.make_async_copy(sens_hbm.at[i], sens.at[i], sens_sem.at[i]) for i in range(fields)
    ]
    for load in sens_loads:
        load.start()
    for_each(devices - 1, greet)

    loads[0].wait()
    loads[1].wait()
    total_wells = wells.shape[1]
    rel = wells[...] - me_c * count
    row_lo = lax.broadcasted_iota(jnp.int32, (rows, total_wells), 0) * layers
    in_row = (rel >= row_lo) & (rel < row_lo + layers)
    lane = wells[...] & (layers - 1)
    at_lane = lax.broadcasted_iota(jnp.int32, (layers, total_wells), 0) == lane
    at_lane = jnp.where(at_lane, 1.0, 0.0).astype(BF16)
    parts = [[], [], []]
    for m in range(members):
        for u in range(unknowns):
            rest = jnp.broadcast_to(misfit[m, u : u + 1, :], (rows, total_wells))
            rest = jnp.where(in_row, rest, 0.0)
            for i in range(3):
                high, rest = split(rest)
                parts[i].append(high.astype(BF16))
    injected = jnp.zeros((fields * rows, layers), F32)
    for piece in parts:
        injected = injected + lax.dot_general(
            jnp.concatenate(piece, axis=0), at_lane, (((1,), (1,)), ((), ())),
            preferred_element_type=F32,
        )
    loads[2].wait()
    source[...] = later[...] + injected.reshape(later.shape)

    def inverse(m, rhs):
        out = None
        for w in range(unknowns):
            term = diag[m, w].astype(F32) * rhs[w][None]
            out = term if out is None else out + term
        return out

    loads[3].wait()
    now = [inverse(m, source[m]) for m in range(members)]
    loads[4].wait()
    loads[5].wait()
    pl.semaphore_wait(barrier, devices - 1)

    first = me_c == 0
    last = me_c == ranks - 1
    next_id = (jnp.minimum(me_c + 1, ranks - 1), me_e)
    prev_id = (jnp.maximum(me_c - 1, 0), me_e)

    def up_copy(k, m):
        return pltpu.make_async_remote_copy(
            src_ref=up_send.at[k, m], dst_ref=below.at[k, m], send_sem=up_ssem.at[k, m],
            recv_sem=up_rsem.at[k, m], device_id=next_id, device_id_type=MESH,
        )

    def down_copy(k, m):
        return pltpu.make_async_remote_copy(
            src_ref=down_send.at[k, m], dst_ref=above.at[k, m], send_sem=down_ssem.at[k, m],
            recv_sem=down_rsem.at[k, m], device_id=prev_id, device_id_type=MESH,
        )

    @pl.when(first)
    def _():
        below[...] = jnp.zeros_like(below)

    @pl.when(last)
    def _():
        above[...] = jnp.zeros_like(above)

    lane_at = lax.broadcasted_iota(jnp.int32, (unknowns, planes, columns, layers), 3)
    col_at = lax.broadcasted_iota(jnp.int32, (unknowns, planes, columns, layers), 2)

    def product(m, k, value, lo, hi):
        out = None
        for u in range(unknowns):
            term = coup[m, k, u, :, lo:hi].astype(F32) * value[u, lo:hi][None]
            out = term if out is None else out + term
        return out

    for k in range(ITERS):
        for m in range(members):
            up_send[k, m] = product(m, 0, now[m], planes - 1, planes)[:, 0]
            down_send[k, m] = product(m, 1, now[m], 0, 1)[:, 0]

            @pl.when(jnp.logical_not(last))
            def _(m=m):
                up_copy(k, m).start()

            @pl.when(jnp.logical_not(first))
            def _(m=m):
                down_copy(k, m).start()

        inner = []
        for m in range(members):
            up = product(m, 0, now[m], 0, planes - 1)
            down = product(m, 1, now[m], 1, planes)
            left = pltpu.roll(product(m, 2, now[m], 0, planes), 1, 2)
            total = jnp.where(col_at == 0, 0.0, left)
            left = pltpu.roll(product(m, 3, now[m], 0, planes), columns - 1, 2)
            total = total + jnp.where(col_at == columns - 1, 0.0, left)
            left = pltpu.roll(product(m, 4, now[m], 0, planes), 1, 3)
            total = total + jnp.where(lane_at == 0, 0.0, left)
            left = pltpu.roll(product(m, 5, now[m], 0, planes), layers - 1, 3)
            total = total + jnp.where(lane_at == layers - 1, 0.0, left)
            inner.append((source[m] - total, up, down))
        if k == 0:
            ids = lax.broadcasted_iota(jnp.int32, (blocks, layers), 0)
            for x in range(planes):
                for y in range(columns):
                    row = x * columns + y
                    hit = jnp.where(bmap[x, y : y + 1, :] == ids, 1.0, 0.0)
                    mask[:, row * layers : (row + 1) * layers] = hit.astype(BF16)
        after = []
        for m in range(members):
            rest, up, down = inner[m]

            @pl.when(jnp.logical_not(first))
            def _(m=m):
                up_copy(k, m).wait_recv()

            @pl.when(jnp.logical_not(last))
            def _(m=m):
                down_copy(k, m).wait_recv()

            rest = rest - jnp.concatenate([below[k, m][:, None], up], axis=1)
            rest = rest - jnp.concatenate([down, above[k, m][:, None]], axis=1)
            after.append(inverse(m, rest))
        now = after

    for m in range(members):
        adj[m] = now[m]
    save = pltpu.make_async_copy(adj, adj_hbm, adj_sem)
    save.start()

    def gather(i, total):
        pltpu.make_async_copy(sens_hbm.at[i], sens.at[i], sens_sem.at[i]).wait()
        high, low = split(adj[i // unknowns, i % unknowns])
        slot = i % 2
        for x in range(planes):
            for y in range(columns):
                row = x * columns + y
                cols = slice(row * layers, (row + 1) * layers)
                hot = mask[:, cols]
                for j, value in enumerate((high, low)):
                    wide = jnp.broadcast_to(value[x, y : y + 1], (16, layers)).astype(BF16)
                    wide = jnp.concatenate([wide] * (blocks // 16), axis=0)
                    lhs[slot, j * blocks : (j + 1) * blocks, cols] = hot * wide
        return total + jnp.dot(
            lhs[slot], sens[i].reshape(count, sens.shape[-1]), preferred_element_type=F32
        )

    total = jnp.zeros((2 * blocks, sens.shape[-1]), F32)
    total = lax.fori_loop(0, fields, gather, total, unroll=blocks <= 64)
    total = total[:blocks] + total[blocks:]
    for c in range(ranks):
        part[c] = total[c * blk_dev : (c + 1) * blk_dev]

    def part_copy(step):
        c, e = other(step)
        return pltpu.make_async_remote_copy(
            src_ref=part.at[c], dst_ref=got.at[step], send_sem=part_ssem, recv_sem=part_rsem,
            device_id=(c, e), device_id_type=MESH,
        )

    for_each(devices - 1, lambda step: part_copy(step).start())
    everything = pltpu.make_async_remote_copy(
        src_ref=got, dst_ref=got, send_sem=part_ssem, recv_sem=part_rsem,
        device_id=next_id, device_id_type=MESH,
    )
    everything.wait_recv()
    grad_ref[...] = part[me_c] + jnp.sum(got[...], axis=0)

    everything.wait_send()
    for k in range(ITERS):
        for m in range(members):
            @pl.when(jnp.logical_not(last))
            def _(k=k, m=m):
                up_copy(k, m).wait_send()

            @pl.when(jnp.logical_not(first))
            def _(k=k, m=m):
                down_copy(k, m).wait_send()

    save.wait()


def solution(mesh):
    ranks, groups = mesh.shape["cells"], mesh.shape["ens"]

    def body(later_adjoint, coupling, diag_inverse, sensitivity, well_cells, well_misfit, block_map):
        members, unknowns, planes, columns, layers = later_adjoint.shape
        params = sensitivity.shape[-1]
        rows = planes * columns
        blk_dev = 4
        blocks = ranks * blk_dev
        fields = members * unknowns
        sens = sensitivity.reshape(fields, rows, layers, params)
        wells = well_cells.reshape(1, -1)
        halo = (ITERS, members, unknowns, columns, layers)
        any_spec = pl.BlockSpec(memory_space=pl.ANY)
        dma = pltpu.SemaphoreType.DMA
        return pl.pallas_call(
            functools.partial(kernel, ranks, groups, blocks),
            out_shape=(
                jax.ShapeDtypeStruct(later_adjoint.shape, F32),
                jax.ShapeDtypeStruct((blk_dev, params), F32),
            ),
            in_specs=[any_spec] * 7,
            out_specs=(any_spec, pl.BlockSpec(memory_space=pltpu.VMEM)),
            scratch_shapes=[
                pltpu.VMEM(later_adjoint.shape, F32),
                pltpu.VMEM(coupling.shape, BF16),
                pltpu.VMEM(diag_inverse.shape, BF16),
                pltpu.VMEM(sens.shape, BF16),
                pltpu.VMEM(wells.shape, jnp.int32),
                pltpu.VMEM(well_misfit.shape, F32),
                pltpu.VMEM(block_map.shape, jnp.int32),
                pltpu.VMEM(later_adjoint.shape, F32),
                pltpu.VMEM(later_adjoint.shape, F32),
                pltpu.VMEM(halo, F32),
                pltpu.VMEM(halo, F32),
                pltpu.VMEM(halo, F32),
                pltpu.VMEM(halo, F32),
                pltpu.VMEM((blocks, rows * layers), BF16),
                pltpu.VMEM((2, 2 * blocks, rows * layers), BF16),
                pltpu.VMEM((ranks, blk_dev, params), F32),
                pltpu.VMEM((ranks * groups - 1, blk_dev, params), F32),
                dma((6,)),
                dma((fields,)),
                dma,
                dma((ITERS, members)),
                dma((ITERS, members)),
                dma((ITERS, members)),
                dma((ITERS, members)),
                dma,
                dma,
            ],
            compiler_params=pltpu.CompilerParams(collective_id=0, has_side_effects=True),
        )(later_adjoint, coupling, diag_inverse, sens, wells, well_misfit, block_map)

    placed = (
        P("ens", None, "cells", None, None),
        P("ens", None, None, None, "cells", None, None),
        P("ens", None, None, "cells", None, None),
        P("ens", None, "cells", None, None, None),
        P(),
        P("ens", None, None),
        P("cells", None, None),
    )
    return jax.shard_map(
        body,
        mesh=mesh,
        in_specs=placed,
        out_specs=(P("ens", None, "cells", None, None), P("cells", None)),
        check_vma=False,
    )
```

```python
import functools

import jax
import jax.numpy as jnp
from jax import lax
from jax.experimental import pallas as pl
from jax.experimental.pallas import tpu as pltpu
from jax.sharding import PartitionSpec as P

ITERS = 4
MESH = pl.DeviceIdType.MESH
F32 = jnp.float32
BF16 = jnp.bfloat16


def for_each(count, step):
    if count <= 64:
        for i in range(count):
            step(i)
    else:
        def body(i, carry):
            step(i)
            return carry

        lax.fori_loop(0, count, body, 0)


def split(value):
    high = value.astype(BF16).astype(F32)
    return high, value - high


def kernel(
    ranks, groups, blocks,
    later_hbm, coup_hbm, diag_hbm, sens_hbm, wells_hbm, misfit_hbm, map_hbm,
    adj, got_out,
    later, coup, diag, sens, wells, misfit, bmap, source,
    up_send, down_send, below, above, mask, lhs, part, got,
    load_sem, sens_sem, up_ssem, up_rsem, down_ssem, down_rsem, part_ssem, part_rsem,
):
    members, unknowns, planes, columns, layers = later.shape
    rows = planes * columns
    count = rows * layers
    devices = ranks * groups
    blk_dev = blocks // ranks
    me_c = lax.axis_index("cells")
    me_e = lax.axis_index("ens")
    me = me_c * groups + me_e

    def other(step):
        at = me + step + 1
        at = jnp.where(at >= devices, at - devices, at)
        return at // groups, at % groups

    barrier = pltpu.get_barrier_semaphore()

    def greet(step):
        c, e = other(step)
        pl.semaphore_signal(barrier, inc=1, device_id=(c, e), device_id_type=MESH)

    loads = [
        pltpu.make_async_copy(src, dst, load_sem.at[i])
        for i, (src, dst) in enumerate(
            [
                (wells_hbm, wells), (misfit_hbm, misfit), (later_hbm, later), (diag_hbm, diag),
                (coup_hbm, coup), (map_hbm, bmap),
            ]
        )
    ]
    for load in loads:
        load.start()
    fields = members * unknowns
    sens_loads = [
        pltpu.make_async_copy(sens_hbm.at[i], sens.at[i], sens_sem.at[i]) for i in range(fields)
    ]
    for load in sens_loads:
        load.start()
    for_each(devices - 1, greet)

    loads[0].wait()
    loads[1].wait()
    total_wells = wells.shape[1]
    rel = wells[...] - me_c * count
    row_lo = lax.broadcasted_iota(jnp.int32, (rows, total_wells), 0) * layers
    in_row = (rel >= row_lo) & (rel < row_lo + layers)
    lane = wells[...] & (layers - 1)
    at_lane = lax.broadcasted_iota(jnp.int32, (layers, total_wells), 0) == lane
    at_lane = jnp.where(at_lane, 1.0, 0.0).astype(BF16)
    parts = [[], [], []]
    for m in range(members):
        for u in range(unknowns):
            rest = jnp.broadcast_to(misfit[m, u : u + 1, :], (rows, total_wells))
            rest = jnp.where(in_row, rest, 0.0)
            for i in range(3):
                high, rest = split(rest)
                parts[i].append(high.astype(BF16))
    injected = jnp.zeros((fields * rows, layers), F32)
    for piece in parts:
        injected = injected + lax.dot_general(
            jnp.concatenate(piece, axis=0), at_lane, (((1,), (1,)), ((), ())),
            preferred_element_type=F32,
        )
    loads[2].wait()
    source[...] = later[...] + injected.reshape(later.shape)

    def inverse(m, rhs):
        out = None
        for w in range(unknowns):
            term = diag[m, w].astype(F32) * rhs[w][None]
            out = term if out is None else out + term
        return out

    loads[3].wait()
    now = [inverse(m, source[m]) for m in range(members)]
    loads[4].wait()

    first = me_c == 0
    last = me_c == ranks - 1
    next_id = (jnp.minimum(me_c + 1, ranks - 1), me_e)
    prev_id = (jnp.maximum(me_c - 1, 0), me_e)

    def up_copy(k, m):
        return pltpu.make_async_remote_copy(
            src_ref=up_send.at[k, m], dst_ref=below.at[k, m], send_sem=up_ssem.at[k, m],
            recv_sem=up_rsem.at[k, m], device_id=next_id, device_id_type=MESH,
        )

    def down_copy(k, m):
        return pltpu.make_async_remote_copy(
            src_ref=down_send.at[k, m], dst_ref=above.at[k, m], send_sem=down_ssem.at[k, m],
            recv_sem=down_rsem.at[k, m], device_id=prev_id, device_id_type=MESH,
        )

    @pl.when(first)
    def _():
        below[...] = jnp.zeros_like(below)

    @pl.when(last)
    def _():
        above[...] = jnp.zeros_like(above)

    lane_at = lax.broadcasted_iota(jnp.int32, (unknowns, planes, columns, layers), 3)
    col_at = lax.broadcasted_iota(jnp.int32, (unknowns, planes, columns, layers), 2)

    def product(m, k, value, lo, hi):
        out = None
        for u in range(unknowns):
            term = coup[m, k, u, :, lo:hi].astype(F32) * value[u, lo:hi][None]
            out = term if out is None else out + term
        return out

    def edges(k, m, value):
        up_send[k, m] = product(m, 0, value, planes - 1, planes)[:, 0]
        down_send[k, m] = product(m, 1, value, 0, 1)[:, 0]

    def send(k, m):
        @pl.when(jnp.logical_not(last))
        def _():
            up_copy(k, m).start()

        @pl.when(jnp.logical_not(first))
        def _():
            down_copy(k, m).start()

    def inside(m, value):
        up = product(m, 0, value, 0, planes - 1)
        down = product(m, 1, value, 1, planes)
        moved = pltpu.roll(product(m, 2, value, 0, planes), 1, 2)
        total = jnp.where(col_at == 0, 0.0, moved)
        moved = pltpu.roll(product(m, 3, value, 0, planes), columns - 1, 2)
        total = total + jnp.where(col_at == columns - 1, 0.0, moved)
        moved = pltpu.roll(product(m, 4, value, 0, planes), 1, 3)
        total = total + jnp.where(lane_at == 0, 0.0, moved)
        moved = pltpu.roll(product(m, 5, value, 0, planes), layers - 1, 3)
        total = total + jnp.where(lane_at == layers - 1, 0.0, moved)
        return source[m] - total, up, down

    for m in range(members):
        edges(0, m, now[m])
    loads[5].wait()
    ids = lax.broadcasted_iota(jnp.int32, (blocks, layers), 0)
    for x in range(planes):
        for y in range(columns):
            row = x * columns + y
            hit = jnp.where(bmap[x, y : y + 1, :] == ids, 1.0, 0.0)
            mask[:, row * layers : (row + 1) * layers] = hit.astype(BF16)
    pl.semaphore_wait(barrier, devices - 1)
    for m in range(members):
        send(0, m)
    for k in range(ITERS):
        inner = [inside(m, now[m]) for m in range(members)]
        after = []
        for m in range(members):
            rest, up, down = inner[m]

            @pl.when(jnp.logical_not(first))
            def _(m=m):
                up_copy(k, m).wait_recv()

            @pl.when(jnp.logical_not(last))
            def _(m=m):
                down_copy(k, m).wait_recv()

            rest = rest - jnp.concatenate([below[k, m][:, None], up], axis=1)
            rest = rest - jnp.concatenate([down, above[k, m][:, None]], axis=1)
            value = inverse(m, rest)
            if k < ITERS - 1:
                edges(k + 1, m, value)
                send(k + 1, m)
            else:
                adj[m] = value
            after.append(value)
        now = after

    def gather(i, total):
        pltpu.make_async_copy(sens_hbm.at[i], sens.at[i], sens_sem.at[i]).wait()
        high, low = split(adj[i // unknowns, i % unknowns])
        slot = i % 2
        for x in range(planes):
            for y in range(columns):
                row = x * columns + y
                cols = slice(row * layers, (row + 1) * layers)
                hot = mask[:, cols]
                for j, value in enumerate((high, low)):
                    wide = jnp.broadcast_to(value[x, y : y + 1], (16, layers)).astype(BF16)
                    wide = jnp.concatenate([wide] * (blocks // 16), axis=0)
                    lhs[slot, j * blocks : (j + 1) * blocks, cols] = hot * wide
        return total + jnp.dot(
            lhs[slot], sens[i].reshape(count, sens.shape[-1]), preferred_element_type=F32
        )

    total = jnp.zeros((2 * blocks, sens.shape[-1]), F32)
    total = lax.fori_loop(0, fields, gather, total, unroll=blocks <= 64)
    total = total[:blocks] + total[blocks:]
    for c in range(ranks):
        part[c] = total[c * blk_dev : (c + 1) * blk_dev]

    def part_copy(step):
        c, e = other(step)
        return pltpu.make_async_remote_copy(
            src_ref=part.at[c], dst_ref=got.at[step], send_sem=part_ssem, recv_sem=part_rsem,
            device_id=(c, e), device_id_type=MESH,
        )

    for_each(devices - 1, lambda step: part_copy(step).start())
    everything = pltpu.make_async_remote_copy(
        src_ref=got, dst_ref=got, send_sem=part_ssem, recv_sem=part_rsem,
        device_id=next_id, device_id_type=MESH,
    )
    everything.wait_recv()
    got_out[...] = part[me_c] + jnp.sum(got[...], axis=0)

    everything.wait_send()
    for k in range(ITERS):
        for m in range(members):
            @pl.when(jnp.logical_not(last))
            def _(k=k, m=m):
                up_copy(k, m).wait_send()

            @pl.when(jnp.logical_not(first))
            def _(k=k, m=m):
                down_copy(k, m).wait_send()


def write_out(adjoint, gradient, adjoint_hbm, gradient_hbm, sem):
    copies = [
        pltpu.make_async_copy(adjoint, adjoint_hbm, sem.at[0]),
        pltpu.make_async_copy(gradient, gradient_hbm, sem.at[1]),
    ]
    for copy in copies:
        copy.start()
    for copy in copies:
        copy.wait()


def solution(mesh):
    ranks, groups = mesh.shape["cells"], mesh.shape["ens"]

    def body(later_adjoint, coupling, diag_inverse, sensitivity, well_cells, well_misfit, block_map):
        members, unknowns, planes, columns, layers = later_adjoint.shape
        params = sensitivity.shape[-1]
        rows = planes * columns
        blk_dev = 4
        blocks = ranks * blk_dev
        fields = members * unknowns
        sens = sensitivity.reshape(fields, rows, layers, params)
        wells = well_cells.reshape(1, -1)
        halo = (ITERS, members, unknowns, columns, layers)
        any_spec = pl.BlockSpec(memory_space=pl.ANY)
        vmem_spec = pl.BlockSpec(memory_space=pltpu.VMEM)
        dma = pltpu.SemaphoreType.DMA
        adjoint, gradient = pl.pallas_call(
            functools.partial(kernel, ranks, groups, blocks),
            out_shape=(
                pltpu.VMEM(later_adjoint.shape, F32),
                pltpu.VMEM((blk_dev, params), F32),
            ),
            in_specs=[any_spec] * 7,
            out_specs=(vmem_spec, vmem_spec),
            scratch_shapes=[
                pltpu.VMEM(later_adjoint.shape, F32),
                pltpu.VMEM(coupling.shape, BF16),
                pltpu.VMEM(diag_inverse.shape, BF16),
                pltpu.VMEM(sens.shape, BF16),
                pltpu.VMEM(wells.shape, jnp.int32),
                pltpu.VMEM(well_misfit.shape, F32),
                pltpu.VMEM(block_map.shape, jnp.int32),
                pltpu.VMEM(later_adjoint.shape, F32),
                pltpu.VMEM(halo, F32),
                pltpu.VMEM(halo, F32),
                pltpu.VMEM(halo, F32),
                pltpu.VMEM(halo, F32),
                pltpu.VMEM((blocks, rows * layers), BF16),
                pltpu.VMEM((2, 2 * blocks, rows * layers), BF16),
                pltpu.VMEM((ranks, blk_dev, params), F32),
                pltpu.VMEM((ranks * groups - 1, blk_dev, params), F32),
                dma((6,)),
                dma((fields,)),
                dma((ITERS, members)),
                dma((ITERS, members)),
                dma((ITERS, members)),
                dma((ITERS, members)),
                dma,
                dma,
            ],
            compiler_params=pltpu.CompilerParams(collective_id=0, has_side_effects=True),
        )(later_adjoint, coupling, diag_inverse, sens, wells, well_misfit, block_map)
        return pl.pallas_call(
            write_out,
            out_shape=(
                jax.ShapeDtypeStruct(adjoint.shape, F32),
                jax.ShapeDtypeStruct(gradient.shape, F32),
            ),
            in_specs=[vmem_spec] * 2,
            out_specs=(any_spec, any_spec),
            scratch_shapes=[dma((2,))],
        )(*[pltpu.with_memory_space_constraint(a, pltpu.VMEM) for a in (adjoint, gradient)])

    placed = (
        P("ens", None, "cells", None, None),
        P("ens", None, None, None, "cells", None, None),
        P("ens", None, None, "cells", None, None),
        P("ens", None, "cells", None, None, None),
        P(),
        P("ens", None, None),
        P("cells", None, None),
    )
    return jax.shard_map(
        body,
        mesh=mesh,
        in_specs=placed,
        out_specs=(P("ens", None, "cells", None, None), P("cells", None)),
        check_vma=False,
    )
```

```python
import functools

import jax
import jax.numpy as jnp
from jax import lax
from jax.experimental import pallas as pl
from jax.experimental.pallas import tpu as pltpu
from jax.sharding import PartitionSpec as P

ITERS = 4
MESH = pl.DeviceIdType.MESH
F32 = jnp.float32
BF16 = jnp.bfloat16


def for_each(count, step):
    if count <= 64:
        for i in range(count):
            step(i)
    else:
        def body(i, carry):
            step(i)
            return carry

        lax.fori_loop(0, count, body, 0)


def split(value):
    high = value.astype(BF16).astype(F32)
    return high, value - high


def kernel(
    ranks, groups, blocks,
    later_hbm, coup_hbm, diag_hbm, sens_hbm, wells_hbm, misfit_hbm, map_hbm,
    adj, got_out,
    later, coup, diag, sens, wells, misfit, bmap, source,
    up_send, down_send, below, above, mask, lhs, part, got,
    load_sem, sens_sem, up_ssem, up_rsem, down_ssem, down_rsem, part_ssem, part_rsem, here_sem,
):
    members, unknowns, planes, columns, layers = later.shape
    rows = planes * columns
    count = rows * layers
    devices = ranks * groups
    blk_dev = blocks // ranks
    me_c = lax.axis_index("cells")
    me_e = lax.axis_index("ens")
    me = me_c * groups + me_e

    def other(step):
        at = me + step + 1
        at = jnp.where(at >= devices, at - devices, at)
        return at // groups, at % groups

    barrier = pltpu.get_barrier_semaphore()

    bits = devices.bit_length() - 1

    def partner(bit):
        size = 1 << bit
        at = me + size - 2 * size * ((me // size) % 2)
        return at // groups, at % groups

    beside = me_c + 2 * (me_c % 2) - 1
    has_beside = (beside >= 0) & (beside < ranks)

    def greet_all():
        @pl.when(has_beside)
        def _():
            pl.semaphore_signal(barrier, inc=1, device_id=(beside, me_e), device_id_type=MESH)

        for bit in range(bits):
            pl.semaphore_signal(barrier, inc=1, device_id=partner(bit), device_id_type=MESH)

    def greeted():
        pl.semaphore_wait(barrier, jnp.where(has_beside, bits + 1, bits))

    def tell(bit):
        if bit < bits:
            pl.semaphore_signal(here_sem.at[bit], inc=1, device_id=partner(bit), device_id_type=MESH)

    def hear(bit):
        if bit < bits:
            pl.semaphore_wait(here_sem.at[bit], 1)

    greet_all()
    loads = [
        pltpu.make_async_copy(src, dst, load_sem.at[i])
        for i, (src, dst) in enumerate(
            [
                (wells_hbm, wells), (misfit_hbm, misfit), (later_hbm, later), (diag_hbm, diag),
                (coup_hbm, coup), (map_hbm, bmap),
            ]
        )
    ]
    for load in loads:
        load.start()
    fields = members * unknowns
    sens_loads = [
        pltpu.make_async_copy(sens_hbm.at[i], sens.at[i], sens_sem.at[i]) for i in range(fields)
    ]

    loads[0].wait()
    loads[1].wait()
    total_wells = wells.shape[1]
    rel = wells[...] - me_c * count
    row_lo = lax.broadcasted_iota(jnp.int32, (rows, total_wells), 0) * layers
    in_row = (rel >= row_lo) & (rel < row_lo + layers)
    lane = wells[...] & (layers - 1)
    at_lane = lax.broadcasted_iota(jnp.int32, (layers, total_wells), 0) == lane
    at_lane = jnp.where(at_lane, 1.0, 0.0).astype(BF16)
    parts = [[], [], []]
    for m in range(members):
        for u in range(unknowns):
            rest = jnp.broadcast_to(misfit[m, u : u + 1, :], (rows, total_wells))
            rest = jnp.where(in_row, rest, 0.0)
            for i in range(3):
                high, rest = split(rest)
                parts[i].append(high.astype(BF16))
    injected = jnp.zeros((fields * rows, layers), F32)
    for piece in parts:
        injected = injected + lax.dot_general(
            jnp.concatenate(piece, axis=0), at_lane, (((1,), (1,)), ((), ())),
            preferred_element_type=F32,
        )
    loads[2].wait()
    source[...] = later[...] + injected.reshape(later.shape)

    def inverse(m, rhs):
        out = None
        for w in range(unknowns):
            term = diag[m, w].astype(F32) * rhs[w][None]
            out = term if out is None else out + term
        return out

    loads[3].wait()
    now = [inverse(m, source[m]) for m in range(members)]
    loads[4].wait()
    for load in sens_loads:
        load.start()

    first = me_c == 0
    last = me_c == ranks - 1
    next_id = (jnp.minimum(me_c + 1, ranks - 1), me_e)
    prev_id = (jnp.maximum(me_c - 1, 0), me_e)

    def up_copy(k, m):
        return pltpu.make_async_remote_copy(
            src_ref=up_send.at[k, m], dst_ref=below.at[k, m], send_sem=up_ssem.at[k, m],
            recv_sem=up_rsem.at[k, m], device_id=next_id, device_id_type=MESH,
        )

    def down_copy(k, m):
        return pltpu.make_async_remote_copy(
            src_ref=down_send.at[k, m], dst_ref=above.at[k, m], send_sem=down_ssem.at[k, m],
            recv_sem=down_rsem.at[k, m], device_id=prev_id, device_id_type=MESH,
        )

    @pl.when(first)
    def _():
        below[...] = jnp.zeros_like(below)

    @pl.when(last)
    def _():
        above[...] = jnp.zeros_like(above)

    lane_at = lax.broadcasted_iota(jnp.int32, (unknowns, planes, columns, layers), 3)
    col_at = lax.broadcasted_iota(jnp.int32, (unknowns, planes, columns, layers), 2)

    def product(m, k, value, lo, hi):
        out = None
        for u in range(unknowns):
            term = coup[m, k, u, :, lo:hi].astype(F32) * value[u, lo:hi][None]
            out = term if out is None else out + term
        return out

    def edges(k, m, value):
        up_send[k, m] = product(m, 0, value, planes - 1, planes)[:, 0]
        down_send[k, m] = product(m, 1, value, 0, 1)[:, 0]

    def send(k, m):
        @pl.when(jnp.logical_not(last))
        def _():
            up_copy(k, m).start()

        @pl.when(jnp.logical_not(first))
        def _():
            down_copy(k, m).start()

    def inside(m, value):
        up = product(m, 0, value, 0, planes - 1)
        down = product(m, 1, value, 1, planes)
        moved = pltpu.roll(product(m, 2, value, 0, planes), 1, 2)
        total = jnp.where(col_at == 0, 0.0, moved)
        moved = pltpu.roll(product(m, 3, value, 0, planes), columns - 1, 2)
        total = total + jnp.where(col_at == columns - 1, 0.0, moved)
        moved = pltpu.roll(product(m, 4, value, 0, planes), 1, 3)
        total = total + jnp.where(lane_at == 0, 0.0, moved)
        moved = pltpu.roll(product(m, 5, value, 0, planes), layers - 1, 3)
        total = total + jnp.where(lane_at == layers - 1, 0.0, moved)
        return source[m] - total, up, down

    for m in range(members):
        edges(0, m, now[m])
    greeted()
    for m in range(members):
        send(0, m)
    tell(0)
    for k in range(ITERS):
        inner = [inside(m, now[m]) for m in range(members)]
        if k == 0:
            loads[5].wait()
            ids = lax.broadcasted_iota(jnp.int32, (blocks, layers), 0)
            for x in range(planes):
                for y in range(columns):
                    row = x * columns + y
                    hit = jnp.where(bmap[x, y : y + 1, :] == ids, 1.0, 0.0)
                    mask[:, row * layers : (row + 1) * layers] = hit.astype(BF16)
        after = []
        for m in range(members):
            rest, up, down = inner[m]

            @pl.when(jnp.logical_not(first))
            def _(m=m):
                up_copy(k, m).wait_recv()

            @pl.when(jnp.logical_not(last))
            def _(m=m):
                down_copy(k, m).wait_recv()

            rest = rest - jnp.concatenate([below[k, m][:, None], up], axis=1)
            rest = rest - jnp.concatenate([down, above[k, m][:, None]], axis=1)
            value = inverse(m, rest)
            if k < ITERS - 1:
                edges(k + 1, m, value)
                send(k + 1, m)
            else:
                adj[m] = value
            after.append(value)
        now = after
        hear(k)
        tell(k + 1)

    def gather(i, total):
        pltpu.make_async_copy(sens_hbm.at[i], sens.at[i], sens_sem.at[i]).wait()
        high, low = split(adj[i // unknowns, i % unknowns])
        slot = i % 2
        for x in range(planes):
            for y in range(columns):
                row = x * columns + y
                cols = slice(row * layers, (row + 1) * layers)
                hot = mask[:, cols]
                for j, value in enumerate((high, low)):
                    wide = jnp.broadcast_to(value[x, y : y + 1], (16, layers)).astype(BF16)
                    wide = jnp.concatenate([wide] * (blocks // 16), axis=0)
                    lhs[slot, j * blocks : (j + 1) * blocks, cols] = hot * wide
        return total + jnp.dot(
            lhs[slot], sens[i].reshape(count, sens.shape[-1]), preferred_element_type=F32
        )

    total = jnp.zeros((2 * blocks, sens.shape[-1]), F32)
    total = lax.fori_loop(0, fields, gather, total, unroll=blocks <= 64)
    total = total[:blocks] + total[blocks:]
    for c in range(ranks):
        part[c] = total[c * blk_dev : (c + 1) * blk_dev]

    def part_copy(step):
        c, e = other(step)
        return pltpu.make_async_remote_copy(
            src_ref=part.at[c], dst_ref=got.at[step], send_sem=part_ssem, recv_sem=part_rsem,
            device_id=(c, e), device_id_type=MESH,
        )

    hear(ITERS)
    for bit in range(ITERS + 1, bits):
        tell(bit)
        hear(bit)
    for_each(devices - 1, lambda step: part_copy(step).start())
    everything = pltpu.make_async_remote_copy(
        src_ref=got, dst_ref=got, send_sem=part_ssem, recv_sem=part_rsem,
        device_id=next_id, device_id_type=MESH,
    )
    everything.wait_recv()
    got_out[...] = part[me_c] + jnp.sum(got[...], axis=0)

    everything.wait_send()
    for k in range(ITERS):
        for m in range(members):
            @pl.when(jnp.logical_not(last))
            def _(k=k, m=m):
                up_copy(k, m).wait_send()

            @pl.when(jnp.logical_not(first))
            def _(k=k, m=m):
                down_copy(k, m).wait_send()


def write_out(adjoint, gradient, adjoint_hbm, gradient_hbm, sem):
    copies = [
        pltpu.make_async_copy(adjoint, adjoint_hbm, sem.at[0]),
        pltpu.make_async_copy(gradient, gradient_hbm, sem.at[1]),
    ]
    for copy in copies:
        copy.start()
    for copy in copies:
        copy.wait()


def solution(mesh):
    ranks, groups = mesh.shape["cells"], mesh.shape["ens"]
    assert (ranks * groups) & (ranks * groups - 1) == 0

    def body(later_adjoint, coupling, diag_inverse, sensitivity, well_cells, well_misfit, block_map):
        members, unknowns, planes, columns, layers = later_adjoint.shape
        params = sensitivity.shape[-1]
        rows = planes * columns
        blk_dev = 4
        blocks = ranks * blk_dev
        fields = members * unknowns
        sens = sensitivity.reshape(fields, rows, layers, params)
        wells = well_cells.reshape(1, -1)
        halo = (ITERS, members, unknowns, columns, layers)
        any_spec = pl.BlockSpec(memory_space=pl.ANY)
        vmem_spec = pl.BlockSpec(memory_space=pltpu.VMEM)
        dma = pltpu.SemaphoreType.DMA
        adjoint, gradient = pl.pallas_call(
            functools.partial(kernel, ranks, groups, blocks),
            out_shape=(
                pltpu.VMEM(later_adjoint.shape, F32),
                pltpu.VMEM((blk_dev, params), F32),
            ),
            in_specs=[any_spec] * 7,
            out_specs=(vmem_spec, vmem_spec),
            scratch_shapes=[
                pltpu.VMEM(later_adjoint.shape, F32),
                pltpu.VMEM(coupling.shape, BF16),
                pltpu.VMEM(diag_inverse.shape, BF16),
                pltpu.VMEM(sens.shape, BF16),
                pltpu.VMEM(wells.shape, jnp.int32),
                pltpu.VMEM(well_misfit.shape, F32),
                pltpu.VMEM(block_map.shape, jnp.int32),
                pltpu.VMEM(later_adjoint.shape, F32),
                pltpu.VMEM(halo, F32),
                pltpu.VMEM(halo, F32),
                pltpu.VMEM(halo, F32),
                pltpu.VMEM(halo, F32),
                pltpu.VMEM((blocks, rows * layers), BF16),
                pltpu.VMEM((2, 2 * blocks, rows * layers), BF16),
                pltpu.VMEM((ranks, blk_dev, params), F32),
                pltpu.VMEM((ranks * groups - 1, blk_dev, params), F32),
                dma((6,)),
                dma((fields,)),
                dma((ITERS, members)),
                dma((ITERS, members)),
                dma((ITERS, members)),
                dma((ITERS, members)),
                dma,
                dma,
                pltpu.SemaphoreType.REGULAR(((ranks * groups).bit_length() - 1,)),
            ],
            compiler_params=pltpu.CompilerParams(collective_id=0, has_side_effects=True),
        )(later_adjoint, coupling, diag_inverse, sens, wells, well_misfit, block_map)
        return pl.pallas_call(
            write_out,
            out_shape=(
                jax.ShapeDtypeStruct(adjoint.shape, F32),
                jax.ShapeDtypeStruct(gradient.shape, F32),
            ),
            in_specs=[vmem_spec] * 2,
            out_specs=(any_spec, any_spec),
            scratch_shapes=[dma((2,))],
        )(*[pltpu.with_memory_space_constraint(a, pltpu.VMEM) for a in (adjoint, gradient)])

    placed = (
        P("ens", None, "cells", None, None),
        P("ens", None, None, None, "cells", None, None),
        P("ens", None, None, "cells", None, None),
        P("ens", None, "cells", None, None, None),
        P(),
        P("ens", None, None),
        P("cells", None, None),
    )
    return jax.shard_map(
        body,
        mesh=mesh,
        in_specs=placed,
        out_specs=(P("ens", None, "cells", None, None), P("cells", None)),
        check_vma=False,
    )
```
